32 devices in a mesh: dp: 8 (over z, x), mp: 4 (over y, core).
Axes of the slice: x: 2, y: 2, z: 4, core: 2. Of those that a mesh axis runs over, the one named last changes fastest.
Arguments:
- hidden_in: bfloat16 [2, 1024, 3584], P(None, 'dp', 'mp'), may hold values from -6 to 6
- out_grad: bfloat16 [2, 1024, 3584], P(None, 'dp', 'mp'), may hold values from -1536 to 1536
- pack_fill: int32 [2, 8], P(None, 'dp'), may hold values from 1 to 128, as said below
- norm_gain: float32 [3584], P('mp'), may hold values from 0.5 to 1.5
- up_weight: bfloat16 [3584, 7168], P(None, 'mp'), may hold values from -0.09375 to 0.09375
- down_weight: bfloat16 [7168, 3584], P('mp'), may hold values from -0.0625 to 0.0625
Outputs:
- in_grad: bfloat16 [2, 1024, 3584], P(None, 'dp', 'mp')
- up_grad: float32 [3584, 7168], P('dp', 'mp')
- down_grad: float32 [7168, 3584], P('mp', 'dp')
- gain_grad: float32 [3584], P('mp')
The draws below stay inside these ranges and needn't reach their ends.
Inputs may be any that keep to these rules, and one draw needn't show every extreme that they name: pack_fill[m, p] real tokens stand at the start of pack p of microbatch m (positions p * 128 onward); the other positions of the pack are padding and carry no loss. In every draw the last pack of the first microbatch is full.
All inputs are finite; a program needn't handle non-finite values.
Results may differ from the reference program's by a relative error of at most 0.014.
Values may be sent and summed in bfloat16 or wider, within the bound.
A program may use at most 128 MiB of HBM per device.

```python
import jax
import jax.numpy as jnp
from jax import lax

D = 3584
FFW = 7168
TOK_DEV = 128
MICRO = 2
TOKENS = 1024
N_MP = 4


def draw_pack_fill(key, part):
    pack_count = TOKENS // TOK_DEV
    pack_pos = jnp.arange(pack_count, dtype=jnp.int32)
    fill_top = TOK_DEV // 16 + 15 * TOK_DEV // 16 * pack_pos * pack_pos // ((pack_count - 1) * (pack_count - 1))
    fill_low = fill_top // 2 + 1
    drawn = jax.random.randint(key, (MICRO, pack_count), fill_low[None, :], fill_top[None, :] + 1, dtype=jnp.int32)
    return drawn.at[0, pack_count - 1].set(TOK_DEV)


def block_scale(stream_key, shape, split, low, top_value):
    def one(dim, shards_of):
        heights = jax.random.uniform(jax.random.fold_in(jax.random.fold_in(stream_key, 6), dim), (shards_of,), jnp.float32, low / len(split), top_value / len(split))
        return jnp.repeat(jnp.exp(heights), shape[dim] // shards_of).reshape((-1,) + (1,) * (len(shape) - dim - 1))

    gain = one(*split[0])
    for cut in split[1:]:
        gain = gain * one(*cut)
    return gain


def normal_values(rng, shape, deviation, most, split=(), kind=jnp.bfloat16):
    loudness = block_scale(rng, shape, split, -0.22, 0.18) if split else 1.0
    entries = jax.random.normal(rng, shape, jnp.float32) * deviation * loudness
    return jnp.minimum(jnp.maximum(entries, -most), most).astype(kind)


def setup_inputs(seed: int = 0) -> dict:
    keys = jax.random.split(jax.random.key(seed), 7)
    hidden_in = normal_values(keys[0], (MICRO, TOKENS, D), 1.0, 6.0, ((1, 8), (2, 4)))
    out_grad = normal_values(keys[1], (MICRO, TOKENS, D), (MICRO * TOKENS // 8), 1536.0, ((1, 8), (2, 4)))
    pack_fill = draw_pack_fill(jax.random.fold_in(keys[6], 71), 0)
    norm_gain = jnp.clip(1.0 + 0.1 * jax.random.normal(keys[3], (D,), jnp.float32), 0.5, 1.5)
    up_weight = normal_values(keys[4], (D, FFW), D ** -0.5, 0.09375, ((1, 4),))
    down_weight = normal_values(keys[5], (FFW, D), FFW ** -0.5, 0.0625, ((0, 4),))
    return {"hidden_in": hidden_in, "out_grad": out_grad, "pack_fill": pack_fill, "norm_gain": norm_gain, "up_weight": up_weight, "down_weight": down_weight}


epsilon = 1e-06

def gelu_tanh(value):
    return jax.nn.gelu(value, approximate=True)

def contract_rows(left, right):
    return lax.dot_general(left, right, (((0,), (0,)), ((), ())), preferred_element_type=jnp.float32)

def contract_cols(left, right):
    return lax.dot_general(left, right, (((1,), (1,)), ((), ())), preferred_element_type=jnp.float32)

def group_sums(grad_pre, up_weight):
    row_count = grad_pre.shape[0]
    model_width = up_weight.shape[0]
    group_width = up_weight.shape[1] // N_MP
    pre_groups = grad_pre.reshape(row_count, N_MP, group_width).transpose(1, 0, 2)
    weight_groups = up_weight.reshape(model_width, N_MP, group_width).transpose(1, 0, 2)

    def add_group(total, pair):
        rounded = contract_cols(pair[0], pair[1]).astype(jnp.bfloat16)
        rounded = lax.optimization_barrier(rounded)
        return (total + rounded.astype(jnp.float32), None)
    total, unused = lax.scan(add_group, jnp.zeros((row_count, model_width), jnp.float32), (pre_groups, weight_groups))
    return total

def micro_grads(hidden_rows, grad_rows, live_mask, inv_count, norm_gain, up_weight, down_weight):
    model_width = hidden_rows.shape[1]
    values = hidden_rows.astype(jnp.float32)
    inv_rms = lax.rsqrt(lax.optimization_barrier(jnp.sum(values * values, axis=1, keepdims=True)) / model_width + epsilon)
    normed = (values * inv_rms * norm_gain[None, :]).astype(jnp.bfloat16)
    pre_act = jnp.dot(normed, up_weight, preferred_element_type=jnp.float32)
    activated = gelu_tanh(pre_act).astype(jnp.bfloat16)
    scaled = (grad_rows.astype(jnp.float32) * live_mask[:, None] * inv_count).astype(jnp.bfloat16)
    grad_act = contract_cols(scaled, down_weight)
    grad_pre = jax.vjp(gelu_tanh, pre_act)[1](grad_act)[0].astype(jnp.bfloat16)
    grad_normed = group_sums(grad_pre, up_weight)
    row_dot = lax.optimization_barrier(jnp.sum(grad_normed * norm_gain[None, :] * values, axis=1, keepdims=True))
    cubed = inv_rms * inv_rms * inv_rms
    in_rows = scaled.astype(jnp.float32) + norm_gain[None, :] * grad_normed * inv_rms - values * cubed * row_dot / model_width
    gain_term = lax.optimization_barrier(jnp.sum(grad_normed * values * inv_rms, axis=0))
    return (in_rows.astype(jnp.bfloat16), contract_rows(normed, grad_pre), contract_rows(activated, scaled), gain_term)

def reference(hidden_in, out_grad, pack_fill, norm_gain, up_weight, down_weight):
    token_total = jnp.sum(pack_fill).astype(jnp.float32)
    inv_count = 1.0 / token_total
    position = jnp.arange(TOKENS, dtype=jnp.int32)
    pack_index = position // TOK_DEV
    offset = position % TOK_DEV
    up_grad = jnp.zeros(up_weight.shape, jnp.float32)
    down_grad = jnp.zeros(down_weight.shape, jnp.float32)
    gain_grad = jnp.zeros(norm_gain.shape, jnp.float32)
    in_parts = []
    for micro_index in range(MICRO):
        live_mask = (offset < pack_fill[micro_index][pack_index]).astype(jnp.float32)
        in_rows, up_term, down_term, gain_term = micro_grads(hidden_in[micro_index], out_grad[micro_index], live_mask, inv_count, norm_gain, up_weight, down_weight)
        up_grad = up_grad + up_term
        down_grad = down_grad + down_term
        gain_grad = gain_grad + gain_term
        in_parts.append(in_rows)
    return (jnp.stack(in_parts), up_grad, down_grad, gain_grad)
```

```python
import functools

import jax
import jax.numpy as jnp
from jax import lax
from jax.experimental import pallas as pl
from jax.experimental.pallas import tpu as pltpu
from jax.sharding import PartitionSpec as P


epsilon = 1e-06


def gelu_tanh(value):
    return jax.nn.gelu(value, approximate=True)


def contract_rows(left, right):
    return lax.dot_general(
        left, right, (((0,), (0,)), ((), ())), preferred_element_type=jnp.float32
    )


def contract_cols(left, right):
    return lax.dot_general(
        left, right, (((1,), (1,)), ((), ())), preferred_element_type=jnp.float32
    )


def stripe(rows, n_dp):
    micro, tok, width = rows.shape
    parts = []
    for m in range(micro):
        part = rows[m].reshape(tok // n_dp, n_dp, width).transpose(1, 0, 2)
        parts.append(part[::-1] if m % 2 else part)
    return jnp.concatenate(parts, axis=1)


def unstripe(slots, micro):
    n_dp, per, width = slots.shape
    share = per // micro
    outs = []
    for m in range(micro):
        part = slots[:, m * share : (m + 1) * share]
        part = part[::-1] if m % 2 else part
        outs.append(part.transpose(1, 0, 2).reshape(share * n_dp, width))
    return jnp.stack(outs)


def flipped(index, bit):
    return index + bit - 2 * bit * lax.rem(lax.div(index, bit), 2)


def flipped_by(index, mask):
    bit = 1
    while bit <= mask:
        if mask & bit:
            index = flipped(index, bit)
        bit *= 2
    return index


def exchange_kernel(axes, *refs):
    count = len(axes)
    ins, outs = refs[:count], refs[count : 2 * count]
    sems = refs[2 * count :]
    barrier = pltpu.get_barrier_semaphore()
    greeted = 0
    for axis in sorted({axis for axis, _ in axes}):
        n, me = lax.axis_size(axis), lax.axis_index(axis)
        for d in range(1, n):
            pl.semaphore_signal(
                barrier,
                inc=1,
                device_id={axis: lax.rem(me + d, n)},
                device_id_type=pl.DeviceIdType.MESH,
            )
        greeted += n - 1
    pl.semaphore_wait(barrier, greeted)

    def send(k, axis, source, target, peer, slot):
        copy = pltpu.make_async_remote_copy(
            src_ref=source,
            dst_ref=outs[k].at[target],
            send_sem=sems[2 * k].at[slot],
            recv_sem=sems[2 * k + 1].at[slot],
            device_id={axis: peer},
            device_id_type=pl.DeviceIdType.MESH,
        )
        copy.start()
        return copy

    trees = [k for k, (_, kind) in enumerate(axes) if kind == "tree"]
    copies = {}

    def forward(k, mask, below):
        axis = axes[k][0]
        me = lax.axis_index(axis)
        owner = flipped_by(me, mask)
        bit = below
        while bit >= 1:
            copies[k, mask ^ bit] = send(
                k,
                axis,
                outs[k].at[owner] if mask else ins[k],
                owner,
                flipped(me, bit),
                mask ^ bit,
            )
            bit //= 2

    for k in trees:
        forward(k, 0, lax.axis_size(axes[k][0]) // 2)
    locals_ = []
    for k, (axis, kind) in enumerate(axes):
        n, me = lax.axis_size(axis), lax.axis_index(axis)
        for d in [n // 2] + [d for d in range(1, n) if d != n // 2]:
            if kind == "tree":
                break
            peer = lax.rem(me + d, n)
            source = ins[k].at[peer] if kind == "split" else ins[k]
            copies[k, d] = send(k, axis, source, me, peer, d)
        own = pltpu.make_async_copy(
            ins[k].at[me] if kind == "split" else ins[k],
            outs[k].at[me],
            sems[2 * k].at[0],
        )
        own.start()
        locals_.append(own)
    relayed = set()
    if trees:
        n = lax.axis_size(axes[trees[0]][0])
        for mask in sorted(range(2, n, 2), key=lambda m: (bin(m).count("1"), -m)):
            for k in trees:
                copies[k, mask].wait_recv()
                relayed.add((k, mask))
                forward(k, mask, (mask & -mask) // 2)
    for key, copy in copies.items():
        copy.wait_send()
        if key not in relayed:
            copy.wait_recv()
    for own in locals_:
        own.wait()


def exchange(arrays, axes, collective_id):
    shapes, sems = [], []
    for array, (axis, kind) in zip(arrays, axes):
        n = lax.axis_size(axis)
        block = array.shape[1:] if kind == "split" else array.shape
        shapes.append(jax.ShapeDtypeStruct((n,) + block, array.dtype))
        sems += [pltpu.SemaphoreType.DMA((n,)), pltpu.SemaphoreType.DMA((n,))]
    vmem = pl.BlockSpec(memory_space=pltpu.VMEM)
    return pl.pallas_call(
        functools.partial(exchange_kernel, axes),
        out_shape=shapes,
        in_specs=[vmem] * len(arrays),
        out_specs=[vmem] * len(arrays),
        scratch_shapes=sems,
        compiler_params=pltpu.CompilerParams(
            collective_id=collective_id, has_side_effects=True
        ),
    )(*arrays)


def on_device(hidden_in, out_grad, pack_fill, norm_gain, up_weight, down_weight):
    micro, tok, width = hidden_in.shape
    model_width, ff_shard = up_weight.shape
    n_dp, n_mp = lax.axis_size("dp"), lax.axis_size("mp")
    me = lax.axis_index("dp")
    share = tok // n_dp
    slot_count = n_dp * micro * share
    chunk = -(-slot_count * 3 // 8 // 16) * 16
    cols = model_width // n_dp

    sent = stripe(jnp.concatenate([hidden_in, out_grad], axis=2), n_dp)
    fill_tile = jnp.broadcast_to(pack_fill, (micro, 128))
    gain_tile = jnp.broadcast_to(norm_gain[None, :], (8, width))
    slots, fills, gain_full = exchange(
        [sent, fill_tile, gain_tile],
        (("dp", "split"), ("dp", "all"), ("mp", "all")),
        0,
    )
    slots = slots.reshape(slot_count, 2 * width)
    fills = fills[:, :, 0].T
    gain_full = gain_full[:, 0, :].reshape(model_width)
    inv_count = 1.0 / jnp.sum(fills).astype(jnp.float32)

    odd = (jnp.arange(micro, dtype=jnp.int32) % 2)[None, :, None]
    steps = jnp.arange(share, dtype=jnp.int32)[None, None, :]
    start = jnp.where(odd == 1, n_dp - 1 - me, me)
    live = (start + steps * n_dp < fills.T[:, :, None]).reshape(slot_count)
    slot_ids = jnp.arange(slot_count, dtype=jnp.int32)
    before = (slot_ids[None, :] < slot_ids[:, None]) & live[None, :]
    place = jnp.where(live, jnp.sum(before.astype(jnp.int32), axis=1), -1)

    ranks = jnp.arange(n_dp, dtype=jnp.int32)[:, None, None]
    starts = jnp.where(odd.reshape(1, micro, 1) == 1, n_dp - 1 - ranks, ranks)
    counts = jnp.clip((fills[None] - starts + n_dp - 1) // n_dp, 0, share)
    most = jnp.max(jnp.sum(counts, axis=(1, 2)))
    chunk_total = (most + chunk - 1) // chunk

    def run_chunk(index):
        spots = jnp.arange(chunk, dtype=jnp.int32) + index * chunk
        pick = (spots[:, None] == place[None, :]).astype(jnp.bfloat16)
        packed = jnp.dot(pick, slots, preferred_element_type=jnp.float32)
        tok_rows = packed[:, :width].astype(jnp.bfloat16)
        scaled = (packed[:, width:] * inv_count).astype(jnp.bfloat16)
        (both,) = exchange(
            [jnp.concatenate([tok_rows, scaled], axis=1)], (("mp", "all"),), 1
        )
        both = both.transpose(1, 0, 2)
        tok_full = both[:, :, :width].reshape(chunk, model_width).astype(jnp.float32)
        scaled_full = both[:, :, width:].reshape(chunk, model_width)
        squares = jnp.sum(tok_full * tok_full, axis=1, keepdims=True)
        inv_rms = lax.rsqrt(squares / model_width + epsilon)
        normed_full = (tok_full * inv_rms * gain_full[None, :]).astype(jnp.bfloat16)
        pre_act = jnp.dot(normed_full, up_weight, preferred_element_type=jnp.float32)
        activated = gelu_tanh(pre_act).astype(jnp.bfloat16)
        grad_act = contract_cols(scaled_full, down_weight)
        grad_pre = jax.vjp(gelu_tanh, pre_act)[1](grad_act)[0].astype(jnp.bfloat16)

        by_cols = jnp.concatenate(
            [
                normed_full.reshape(chunk, n_dp, cols),
                scaled_full.reshape(chunk, n_dp, cols),
            ],
            axis=2,
        ).transpose(1, 0, 2)

        row_part = jnp.sum(grad_pre.astype(jnp.float32) * pre_act, axis=1, keepdims=True)
        partial = contract_cols(grad_pre, up_weight).astype(jnp.bfloat16)
        shares, row_parts = exchange(
            [
                partial.reshape(chunk, n_mp, width).transpose(1, 0, 2),
                jnp.broadcast_to(row_part / inv_rms, (chunk, 128)),
            ],
            (("mp", "split"), ("mp", "all")),
            2,
        )
        grad_normed = jnp.sum(shares.astype(jnp.float32), axis=0)
        row_dot = jnp.sum(row_parts, axis=0)[:, :1]
        values = tok_rows.astype(jnp.float32)
        cubed = inv_rms * inv_rms * inv_rms
        in_rows = (
            scaled.astype(jnp.float32)
            + norm_gain[None, :] * grad_normed * inv_rms
            - values * cubed * row_dot / model_width
        ).astype(jnp.bfloat16)
        gain_term = jnp.sum(grad_normed * values * inv_rms, axis=0)
        back = contract_rows(pick, in_rows).astype(jnp.bfloat16)
        act_all, pre_all, by_cols, back, gain_parts = exchange(
            [
                activated,
                grad_pre,
                by_cols,
                back.reshape(n_dp, micro * share, width),
                jnp.broadcast_to(gain_term[None, :], (8, width)),
            ],
            (("dp", "tree"), ("dp", "tree"), ("dp", "split"), ("dp", "split"), ("dp", "all")),
            3,
        )
        by_cols = by_cols.reshape(n_dp * chunk, 2 * cols)
        up_term = contract_rows(by_cols[:, :cols], pre_all.reshape(n_dp * chunk, ff_shard))
        down_term = contract_rows(act_all.reshape(n_dp * chunk, ff_shard), by_cols[:, cols:])
        return (back, up_term, down_term, jnp.sum(gain_parts[:, 0], axis=0))

    def add_chunk(index, total):
        return jax.tree.map(jnp.add, total, run_chunk(index))

    total = run_chunk(jnp.int32(0))
    back, up_grad, down_grad, gain_acc = lax.fori_loop(1, chunk_total, add_chunk, total)
    return (unstripe(back, micro), up_grad, down_grad, gain_acc)


gelu_slope = 0.7978845608028654
gelu_cube = 0.044715
MESH = pl.DeviceIdType.MESH


def packed_chunk(slot_count):
    return -(-slot_count * 3 // 8 // 16) * 16


def fused_kernel(
    hid, og, fill, gain, index, up_hbm, down_hbm,
    in_part, up_out, down_out, gain_out, fills_out,
    upw, dnw, hbuf, gbuf, act, pre, normed, nsl, gsl, gp_own,
    sent_h, sent_g, got_h, got_g, fill_send, gain_send, gain_full,
    part, shares, row_send, rows_in, term_send, terms_in,
    sent_back, got_back, perm, pick,
    w_sem, h0_s, h0_r, g0_s, g0_r, f_s, f_r, n_s, n_r,
    ht_s, ht_r, gt_s, gt_r, p_s, p_r, q_s, q_r, b_s, b_r, t_s, t_r,
):
    n_dp, n_mp = lax.axis_size("dp"), lax.axis_size("mp")
    me, mine = lax.axis_index("dp"), lax.axis_index("mp")
    core = lax.rem(mine, 2)
    high = lax.div(mine, 2)
    low = lax.rem(me, 2)
    micro, tok, width = hid.shape
    model, ff = upw.shape
    rows = micro * tok
    share = tok // n_dp
    per = micro * share
    chunk = hbuf.shape[0] // n_dp
    cols = model // n_dp
    group = 2 * chunk
    tile = 256
    f32, bf16 = jnp.float32, jnp.bfloat16

    loads = [
        pltpu.make_async_copy(up_hbm, upw, w_sem.at[0]),
        pltpu.make_async_copy(down_hbm, dnw, w_sem.at[1]),
    ]
    for load in loads:
        load.start()

    barrier = pltpu.get_barrier_semaphore()
    for axis, n, at in (("dp", n_dp, me), ("mp", n_mp, mine)):
        for d in range(1, n):
            pl.semaphore_signal(
                barrier, inc=1, device_id={axis: lax.rem(at + d, n)}, device_id_type=MESH
            )

    shift = share.bit_length() - 1
    line = lax.broadcasted_iota(jnp.int32, (rows, rows), 0)
    lane = lax.broadcasted_iota(jnp.int32, (rows, rows), 1)
    m_of = (line >> shift) & (micro - 1)
    d_of = line >> (per.bit_length() - 1)
    first = jnp.where((m_of & 1) == 1, n_dp - 1 - d_of, d_of)
    source = m_of * tok + (line & (share - 1)) * n_dp + first
    perm[...] = (source == lane).astype(f32).astype(bf16)
    for block, target in ((hid, sent_h), (og, sent_g)):
        for m in range(micro):
            piece = jnp.dot(
                perm[:, m * tok : (m + 1) * tok], block[m], preferred_element_type=f32
            )
            if m == 0:
                total = piece
            else:
                total = total + piece
        target[...] = total.astype(bf16)
    ids = lax.broadcasted_iota(jnp.int32, fill_send.shape, 0)
    tile_fill = jnp.zeros(fill_send.shape, jnp.int32)
    for m in range(micro):
        tile_fill = jnp.where(ids == m, fill[m, 0], tile_fill)
    fill_send[...] = tile_fill
    gain_send[...] = jnp.broadcast_to(gain[...], gain_send.shape)

    pl.semaphore_wait(barrier, n_dp + n_mp - 2)

    sent = []

    def ship(src, dst, s_sem, r_sem, device):
        copy = pltpu.make_async_remote_copy(
            src_ref=src, dst_ref=dst, send_sem=s_sem, recv_sem=r_sem,
            device_id=device, device_id_type=MESH,
        )
        copy.start()
        sent.append(copy)
        return copy

    def to_dp(source_of, target, s_sems, r_sems):
        out = []
        for d in [n_dp // 2] + [d for d in range(1, n_dp) if d != n_dp // 2]:
            peer = lax.rem(me + d, n_dp)
            out.append(ship(source_of(peer), target, s_sems.at[d], r_sems.at[d], {"dp": peer}))
        return out

    def to_mp(source_of, target, s_sems, r_sems):
        out = []
        for d in range(1, n_mp):
            peer = lax.rem(mine + d, n_mp)
            out.append(ship(source_of(peer), target, s_sems.at[d], r_sems.at[d], {"mp": peer}))
        return out

    def slot(ref, r):
        return ref.at[pl.ds(pl.multiple_of(r * per, per), per), :]

    def strip(q):
        return pl.ds(pl.multiple_of(q * width, 128), width)

    def rank_rows(r):
        return pl.ds(pl.multiple_of(r * chunk, 16), chunk)

    fill_copies = to_dp(lambda peer: fill_send, fills_out.at[me], f_s, f_r)
    h_copies = to_dp(lambda peer: slot(sent_h, peer), slot(got_h, me), h0_s, h0_r)
    gain_copies = to_mp(lambda peer: gain_send, gain_full.at[:, strip(mine)], n_s, n_r)
    g_copies = to_dp(lambda peer: slot(sent_g, peer), slot(got_g, me), g0_s, g0_r)
    here = pl.ds(pl.multiple_of(me * per, per), per)
    got_h[here, :] = sent_h[here, :]
    got_g[here, :] = sent_g[here, :]
    fills_out[me] = fill_send[...]
    gain_full[:, strip(mine)] = gain_send[...]

    for copy in fill_copies:
        copy.wait_recv()
    lanes = lax.broadcasted_iota(jnp.int32, (1, rows), 1)
    count = jnp.zeros((1, rows), jnp.int32)
    token_total = jnp.zeros((1, 1), jnp.int32)
    for r in range(n_dp):
        for m in range(micro):
            one = fills_out[r, m : m + 1, 0:1]
            token_total = token_total + one
            count = jnp.where((lanes >> shift) == r * micro + m, one, count)
    odd = (lanes >> shift) & 1
    begin = jnp.where(odd == 1, n_dp - 1 - me, me)
    live = begin + (lanes & (share - 1)) * n_dp < count
    inv_count = 1.0 / token_total.astype(f32)
    live_f = live.astype(f32)
    upto = (line < lane).astype(f32).astype(bf16)
    place = jnp.dot(
        jnp.broadcast_to(live_f, (16, rows)).astype(bf16), upto, preferred_element_type=f32
    )[0:1, :]
    place = jnp.where(live, place, -1.0)
    spots = (lax.broadcasted_iota(jnp.int32, (chunk, rows), 0) + index[0] * chunk).astype(f32)
    pick[...] = (spots == place).astype(f32).astype(bf16)

    def along(at_dp, at_mp, x, y):
        return (
            at_dp + x - 2 * x * lax.rem(at_dp, 2),
            at_mp + 2 * y - 4 * y * lax.div(at_mp, 2),
        )

    def owner(t, at_mp, c):
        t1, t0 = (t >> 1) & 1, t & 1
        x = t1 * (1 - c) + t0 * c
        y = t0 * (1 - c) + t1 * c
        return along(flipped_by(me, (t >> 2) * 2), at_mp, x, y)

    def toward(bit):
        if bit >= 4:
            return flipped(me, bit // 2), mine
        if bit == 2:
            return along(me, mine, 1 - core, core)
        return along(me, mine, core, 1 - core)

    nodes = 2 * n_dp
    top = n_dp
    partner = mine + 1 - 2 * core
    trees = {"h": (hbuf, ht_s, ht_r), "g": (gbuf, gt_s, gt_r)}
    tree_copies = {}

    def forward(k, t):
        buf, s_sems, r_sems = trees[k]
        dp_o, mp_o = owner(t, mine, core)
        place_ = buf.at[rank_rows(dp_o), strip(mp_o)]
        bit = (t & -t) // 2 if t else top
        while bit >= 1:
            dp_t, mp_t = toward(bit)
            tree_copies[k, t ^ bit] = ship(
                place_, place_, s_sems.at[t ^ bit], r_sems.at[t ^ bit], {"dp": dp_t, "mp": mp_t}
            )
            bit //= 2
        tree_copies[k, nodes + t] = ship(
            place_, place_, s_sems.at[nodes + t], r_sems.at[nodes + t], {"mp": partner}
        )

    def arrive(k, *ts):
        for t in ts:
            tree_copies[k, t].wait_recv()
            forward(k, t)

    def joined(k, z):
        for t in range(4 * z, 4 * z + 4):
            tree_copies[k, nodes + t].wait_recv()

    def base_of(z):
        return 2 * flipped_by(lax.div(me, 2), z)

    half = lax.div(me, n_dp // n_mp)
    part_at = lax.rem(me, n_dp // n_mp)

    def slice_cols(value):
        out = value[:, 0:cols]
        for i in range(1, n_dp // n_mp):
            out = jnp.where(part_at == i, value[:, i * cols : (i + 1) * cols], out)
        return out

    def rms(block):
        return lax.rsqrt(jnp.sum(block * block, axis=1, keepdims=True) / model + epsilon)

    def do_pre(z):
        joined("h", z)
        base = base_of(z)

        def norm_rows(i, carry):
            src = pl.ds(pl.multiple_of(base * chunk + i * 16, 16), 16)
            dst = pl.ds(pl.multiple_of(i * 16, 16), 16)
            value = hbuf[src, :].astype(f32)
            normed[dst, :] = (value * rms(value) * gain_full[0:1, :]).astype(bf16)
            return carry

        lax.fori_loop(0, group // 16, norm_rows, 0)
        nsl[z] = slice_cols(normed[:, strip(half)].astype(f32)).astype(bf16)

        def pre_tile(n, carry):
            at = pl.ds(pl.multiple_of(n * tile, tile), tile)
            value = jnp.dot(normed[...], upw[:, at], preferred_element_type=f32)
            pre[z, :, at] = value
            bent = jnp.tanh(gelu_slope * (value + gelu_cube * (value * value * value)))
            act[z, :, at] = (value * (0.5 * (1.0 + bent))).astype(bf16)
            return carry

        lax.fori_loop(0, ff // tile, pre_tile, 0)

    def do_grad(z):
        joined("g", z)
        base = base_of(z)
        block = pl.ds(pl.multiple_of(base * chunk, 16), group)
        gsl[...] = slice_cols(gbuf[block, strip(half)].astype(f32)).astype(bf16)

        def grad_tile(n, carry):
            at = pl.ds(pl.multiple_of(n * tile, tile), tile)
            grad = contract_cols(gbuf[block, :], dnw[at, :])
            value = pre[z, :, at]
            square = value * value
            bent = jnp.tanh(gelu_slope * (value + gelu_cube * (square * value)))
            slope = 0.5 * (1.0 + bent) + (0.5 * value) * (1.0 - bent * bent) * (
                gelu_slope * (1.0 + 3.0 * gelu_cube * square)
            )
            back = (grad * slope).astype(bf16)
            if z == 0:
                gp_own[:, at] = back
            up_term = contract_rows(nsl[z], back)
            down_term = contract_rows(act[z, :, at], gsl[...])
            if z == 0:
                up_out[:, at] = up_term
                down_out[at, :] = down_term
            else:
                up_out[:, at] += up_term
                down_out[at, :] += down_term
            return carry

        lax.fori_loop(0, ff // tile, grad_tile, 0)

    def compact(got, buf, scale):
        packed = jnp.dot(pick[...], got[...], preferred_element_type=f32)
        if scale is not None:
            packed = packed * scale
        buf[rank_rows(me), strip(mine)] = packed.astype(bf16)

    for copy in h_copies:
        copy.wait_recv()
    compact(got_h, hbuf, None)
    forward("h", 0)
    for copy in gain_copies:
        copy.wait_recv()
    arrive("h", 8, 4, 2, 1)
    for copy in g_copies:
        copy.wait_recv()
    compact(got_g, gbuf, inv_count)
    forward("g", 0)
    arrive("h", 12, 3, 6, 10)
    loads[0].wait()
    do_pre(0)
    arrive("h", 14, 5, 7)
    arrive("g", 8, 4)
    do_pre(1)
    arrive("h", 9, 11)
    arrive("g", 2, 1)
    do_pre(2)
    arrive("h", 13, 15)
    arrive("g", 12)
    do_pre(3)
    arrive("g", 3, 6, 10)
    loads[1].wait()
    do_grad(0)

    own = pl.ds(pl.multiple_of(low * chunk, 16), chunk)
    own_gp = gp_own[own, :]
    own_pre = pre[0, own, :]
    inv_rms = rms(hbuf[rank_rows(me), :].astype(f32))
    row_part = jnp.sum(own_gp.astype(f32) * own_pre, axis=1, keepdims=True)
    row_send[...] = jnp.broadcast_to(row_part / inv_rms, row_send.shape)

    def part_tile(n, carry):
        at = pl.ds(pl.multiple_of(n * tile, tile), tile)
        part[:, at] = contract_cols(gp_own[own, :], upw[at, :]).astype(bf16)
        return carry

    lax.fori_loop(0, model // tile, part_tile, 0)
    part_copies = to_mp(lambda peer: part.at[:, strip(peer)], shares.at[mine], p_s, p_r)
    part_copies += to_mp(lambda peer: row_send, rows_in.at[mine], q_s, q_r)

    arrive("g", 14, 5, 7)
    do_grad(1)

    for copy in part_copies:
        copy.wait_recv()
    grad_normed = part[:, strip(mine)].astype(f32)
    row_dot = row_send[:, 0:1]
    for d in range(1, n_mp):
        peer = lax.rem(mine + d, n_mp)
        grad_normed = grad_normed + shares[peer].astype(f32)
        row_dot = row_dot + rows_in[peer][:, 0:1]
    values = hbuf[rank_rows(me), strip(mine)].astype(f32)
    scaled = gbuf[rank_rows(me), strip(mine)].astype(f32)
    cubed = inv_rms * inv_rms * inv_rms
    in_rows = (
        scaled + gain[...] * grad_normed * inv_rms - values * (cubed * row_dot / model)
    ).astype(bf16)
    gain_term = jnp.sum(grad_normed * values * inv_rms, axis=0, keepdims=True)
    term_send[...] = jnp.broadcast_to(gain_term, term_send.shape)
    terms_in[me] = term_send[...]
    back = contract_rows(pick[...], in_rows).astype(bf16)
    sent_back[...] = back
    got_back[here, :] = sent_back[here, :]
    back_copies = to_dp(lambda peer: slot(sent_back, peer), slot(got_back, me), b_s, b_r)
    back_copies += to_dp(lambda peer: term_send, terms_in.at[me], t_s, t_r)

    arrive("g", 9, 11)
    do_grad(2)
    arrive("g", 13, 15)
    do_grad(3)

    for copy in back_copies:
        copy.wait_recv()
    gain_out[...] = jnp.sum(terms_in[...], axis=0)
    for m in range(micro):
        in_part[m] = contract_rows(perm[:, m * tok : (m + 1) * tok], got_back[...]).astype(bf16)
    for copy in sent:
        copy.wait_send()


def fused_call(hidden_in, out_grad, pack_fill, norm_gain, index, up_weight, down_weight):
    micro, tok, width = hidden_in.shape
    model, ff = up_weight.shape
    n_dp, n_mp = lax.axis_size("dp"), lax.axis_size("mp")
    rows = micro * tok
    per = rows // n_dp
    chunk = packed_chunk(rows)
    cols = model // n_dp
    group = 2 * chunk
    zs = n_dp // 2
    f32, bf16 = jnp.float32, jnp.bfloat16
    vmem = pl.BlockSpec(memory_space=pltpu.VMEM)
    smem = pl.BlockSpec(memory_space=pltpu.SMEM)
    hbm = pl.BlockSpec(memory_space=pl.ANY)
    dma = pltpu.SemaphoreType.DMA
    return pl.pallas_call(
        fused_kernel,
        out_shape=[
            jax.ShapeDtypeStruct((micro, tok, width), bf16),
            jax.ShapeDtypeStruct((cols, ff), f32),
            jax.ShapeDtypeStruct((ff, cols), f32),
            jax.ShapeDtypeStruct((8, width), f32),
            jax.ShapeDtypeStruct((n_dp, 8, 128), jnp.int32),
        ],
        in_specs=[vmem, vmem, smem, vmem, smem, hbm, hbm],
        out_specs=[vmem] * 5,
        scratch_shapes=[
            pltpu.VMEM((model, ff), bf16),
            pltpu.VMEM((ff, model), bf16),
            pltpu.VMEM((n_dp * chunk, model), bf16),
            pltpu.VMEM((n_dp * chunk, model), bf16),
            pltpu.VMEM((zs, group, ff), bf16),
            pltpu.VMEM((zs, group, ff), f32),
            pltpu.VMEM((group, model), bf16),
            pltpu.VMEM((zs, group, cols), bf16),
            pltpu.VMEM((group, cols), bf16),
            pltpu.VMEM((group, ff), bf16),
            pltpu.VMEM((rows, width), bf16),
            pltpu.VMEM((rows, width), bf16),
            pltpu.VMEM((rows, width), bf16),
            pltpu.VMEM((rows, width), bf16),
            pltpu.VMEM((8, 128), jnp.int32),
            pltpu.VMEM((8, width), f32),
            pltpu.VMEM((8, model), f32),
            pltpu.VMEM((chunk, model), bf16),
            pltpu.VMEM((n_mp, chunk, width), bf16),
            pltpu.VMEM((chunk, 128), f32),
            pltpu.VMEM((n_mp, chunk, 128), f32),
            pltpu.VMEM((8, width), f32),
            pltpu.VMEM((n_dp, 8, width), f32),
            pltpu.VMEM((rows, width), bf16),
            pltpu.VMEM((rows, width), bf16),
            pltpu.VMEM((rows, rows), bf16),
            pltpu.VMEM((chunk, rows), bf16),
            dma((2,)),
        ]
        + [dma((n_dp,))] * 6
        + [dma((n_mp,))] * 2
        + [dma((4 * n_dp,))] * 4
        + [dma((n_mp,))] * 4
        + [dma((n_dp,))] * 4,
        compiler_params=pltpu.CompilerParams(
            collective_id=7, has_side_effects=True, vmem_limit_bytes=67043328
        ),
        cost_estimate=pl.CostEstimate(
            flops=8 * rows * model * ff, bytes_accessed=6 * model * ff, transcendentals=0
        ),
    )(hidden_in, out_grad, pack_fill, norm_gain[None, :], index, up_weight, down_weight)


def on_device_fused(hidden_in, out_grad, pack_fill, norm_gain, up_weight, down_weight):
    micro, tok, _ = hidden_in.shape
    n_dp = lax.axis_size("dp")
    share = tok // n_dp
    chunk = packed_chunk(micro * tok)

    def run_chunk(index):
        return fused_call(
            hidden_in, out_grad, pack_fill, norm_gain,
            jnp.reshape(index, (1,)).astype(jnp.int32), up_weight, down_weight,
        )

    *total, fills = run_chunk(jnp.int32(0))
    fills = fills[:, :micro, 0].T
    odd = (jnp.arange(micro, dtype=jnp.int32) % 2).reshape(1, micro, 1)
    ranks = jnp.arange(n_dp, dtype=jnp.int32)[:, None, None]
    starts = jnp.where(odd == 1, n_dp - 1 - ranks, ranks)
    counts = jnp.clip((fills[None] - starts + n_dp - 1) // n_dp, 0, share)
    most = jnp.max(jnp.sum(counts, axis=(1, 2)))
    chunk_total = (most + chunk - 1) // chunk

    def add_chunk(index, so_far):
        *more, _ = run_chunk(index)
        return jax.tree.map(jnp.add, so_far, more)

    in_grad, up_grad, down_grad, gain = lax.fori_loop(1, chunk_total, add_chunk, total)
    return (in_grad, up_grad, down_grad, gain[0])


def solution(mesh):
    in_specs = (
        P(None, "dp", "mp"),
        P(None, "dp", "mp"),
        P(None, "dp"),
        P("mp"),
        P(None, "mp"),
        P("mp", None),
    )
    out_specs = (P(None, "dp", "mp"), P("dp", "mp"), P("mp", "dp"), P("mp"))

    def local(hidden_in, out_grad, pack_fill, norm_gain, up_weight, down_weight):
        micro, tok, width = hidden_in.shape
        n_dp, n_mp = mesh.shape["dp"], mesh.shape["mp"]
        share = tok // n_dp
        fits = (
            (n_dp, n_mp, micro) == (8, 4, 2)
            and width % 128 == 0
            and up_weight.shape[1] % 256 == 0
            and up_weight.shape[0] % 256 == 0
            and tok % 128 == 0
            and share & (share - 1) == 0
        )
        body = on_device_fused if fits else on_device
        return body(hidden_in, out_grad, pack_fill, norm_gain, up_weight, down_weight)

    return jax.shard_map(
        local, mesh=mesh, in_specs=in_specs, out_specs=out_specs, check_vma=False
    )
```

```python
import contextlib
import functools

import jax
import jax.numpy as jnp
from jax import lax
from jax.experimental import pallas as pl
from jax.experimental.pallas import tpu as pltpu
from jax.sharding import PartitionSpec as P


epsilon = 1e-06


def gelu_tanh(value):
    return jax.nn.gelu(value, approximate=True)


def contract_rows(left, right):
    return lax.dot_general(
        left, right, (((0,), (0,)), ((), ())), preferred_element_type=jnp.float32
    )


def contract_cols(left, right):
    return lax.dot_general(
        left, right, (((1,), (1,)), ((), ())), preferred_element_type=jnp.float32
    )


def stripe(rows, n_dp):
    micro, tok, width = rows.shape
    parts = []
    for m in range(micro):
        part = rows[m].reshape(tok // n_dp, n_dp, width).transpose(1, 0, 2)
        parts.append(part[::-1] if m % 2 else part)
    return jnp.concatenate(parts, axis=1)


def unstripe(slots, micro):
    n_dp, per, width = slots.shape
    share = per // micro
    outs = []
    for m in range(micro):
        part = slots[:, m * share : (m + 1) * share]
        part = part[::-1] if m % 2 else part
        outs.append(part.transpose(1, 0, 2).reshape(share * n_dp, width))
    return jnp.stack(outs)


def flipped(index, bit):
    return index + bit - 2 * bit * lax.rem(lax.div(index, bit), 2)


def flipped_by(index, mask):
    bit = 1
    while bit <= mask:
        if mask & bit:
            index = flipped(index, bit)
        bit *= 2
    return index


def exchange_kernel(axes, *refs):
    count = len(axes)
    ins, outs = refs[:count], refs[count : 2 * count]
    sems = refs[2 * count :]
    barrier = pltpu.get_barrier_semaphore()
    greeted = 0
    for axis in sorted({axis for axis, _ in axes}):
        n, me = lax.axis_size(axis), lax.axis_index(axis)
        for d in range(1, n):
            pl.semaphore_signal(
                barrier,
                inc=1,
                device_id={axis: lax.rem(me + d, n)},
                device_id_type=pl.DeviceIdType.MESH,
            )
        greeted += n - 1
    pl.semaphore_wait(barrier, greeted)

    def send(k, axis, source, target, peer, slot):
        copy = pltpu.make_async_remote_copy(
            src_ref=source,
            dst_ref=outs[k].at[target],
            send_sem=sems[2 * k].at[slot],
            recv_sem=sems[2 * k + 1].at[slot],
            device_id={axis: peer},
            device_id_type=pl.DeviceIdType.MESH,
        )
        copy.start()
        return copy

    trees = [k for k, (_, kind) in enumerate(axes) if kind == "tree"]
    copies = {}

    def forward(k, mask, below):
        axis = axes[k][0]
        me = lax.axis_index(axis)
        owner = flipped_by(me, mask)
        bit = below
        while bit >= 1:
            copies[k, mask ^ bit] = send(
                k,
                axis,
                outs[k].at[owner] if mask else ins[k],
                owner,
                flipped(me, bit),
                mask ^ bit,
            )
            bit //= 2

    for k in trees:
        forward(k, 0, lax.axis_size(axes[k][0]) // 2)
    locals_ = []
    for k, (axis, kind) in enumerate(axes):
        n, me = lax.axis_size(axis), lax.axis_index(axis)
        for d in [n // 2] + [d for d in range(1, n) if d != n // 2]:
            if kind == "tree":
                break
            peer = lax.rem(me + d, n)
            source = ins[k].at[peer] if kind == "split" else ins[k]
            copies[k, d] = send(k, axis, source, me, peer, d)
        own = pltpu.make_async_copy(
            ins[k].at[me] if kind == "split" else ins[k],
            outs[k].at[me],
            sems[2 * k].at[0],
        )
        own.start()
        locals_.append(own)
    relayed = set()
    if trees:
        n = lax.axis_size(axes[trees[0]][0])
        for mask in sorted(range(2, n, 2), key=lambda m: (bin(m).count("1"), -m)):
            for k in trees:
                copies[k, mask].wait_recv()
                relayed.add((k, mask))
                forward(k, mask, (mask & -mask) // 2)
    for key, copy in copies.items():
        copy.wait_send()
        if key not in relayed:
            copy.wait_recv()
    for own in locals_:
        own.wait()


def exchange(arrays, axes, collective_id):
    shapes, sems = [], []
    for array, (axis, kind) in zip(arrays, axes):
        n = lax.axis_size(axis)
        block = array.shape[1:] if kind == "split" else array.shape
        shapes.append(jax.ShapeDtypeStruct((n,) + block, array.dtype))
        sems += [pltpu.SemaphoreType.DMA((n,)), pltpu.SemaphoreType.DMA((n,))]
    vmem = pl.BlockSpec(memory_space=pltpu.VMEM)
    return pl.pallas_call(
        functools.partial(exchange_kernel, axes),
        out_shape=shapes,
        in_specs=[vmem] * len(arrays),
        out_specs=[vmem] * len(arrays),
        scratch_shapes=sems,
        compiler_params=pltpu.CompilerParams(
            collective_id=collective_id, has_side_effects=True
        ),
    )(*arrays)


def on_device(hidden_in, out_grad, pack_fill, norm_gain, up_weight, down_weight):
    micro, tok, width = hidden_in.shape
    model_width, ff_shard = up_weight.shape
    n_dp, n_mp = lax.axis_size("dp"), lax.axis_size("mp")
    me = lax.axis_index("dp")
    share = tok // n_dp
    slot_count = n_dp * micro * share
    chunk = -(-slot_count * 3 // 8 // 16) * 16
    cols = model_width // n_dp

    sent = stripe(jnp.concatenate([hidden_in, out_grad], axis=2), n_dp)
    fill_tile = jnp.broadcast_to(pack_fill, (micro, 128))
    gain_tile = jnp.broadcast_to(norm_gain[None, :], (8, width))
    slots, fills, gain_full = exchange(
        [sent, fill_tile, gain_tile],
        (("dp", "split"), ("dp", "all"), ("mp", "all")),
        0,
    )
    slots = slots.reshape(slot_count, 2 * width)
    fills = fills[:, :, 0].T
    gain_full = gain_full[:, 0, :].reshape(model_width)
    inv_count = 1.0 / jnp.sum(fills).astype(jnp.float32)

    odd = (jnp.arange(micro, dtype=jnp.int32) % 2)[None, :, None]
    steps = jnp.arange(share, dtype=jnp.int32)[None, None, :]
    start = jnp.where(odd == 1, n_dp - 1 - me, me)
    live = (start + steps * n_dp < fills.T[:, :, None]).reshape(slot_count)
    slot_ids = jnp.arange(slot_count, dtype=jnp.int32)
    before = (slot_ids[None, :] < slot_ids[:, None]) & live[None, :]
    place = jnp.where(live, jnp.sum(before.astype(jnp.int32), axis=1), -1)

    ranks = jnp.arange(n_dp, dtype=jnp.int32)[:, None, None]
    starts = jnp.where(odd.reshape(1, micro, 1) == 1, n_dp - 1 - ranks, ranks)
    counts = jnp.clip((fills[None] - starts + n_dp - 1) // n_dp, 0, share)
    most = jnp.max(jnp.sum(counts, axis=(1, 2)))
    chunk_total = (most + chunk - 1) // chunk

    def run_chunk(index):
        spots = jnp.arange(chunk, dtype=jnp.int32) + index * chunk
        pick = (spots[:, None] == place[None, :]).astype(jnp.bfloat16)
        packed = jnp.dot(pick, slots, preferred_element_type=jnp.float32)
        tok_rows = packed[:, :width].astype(jnp.bfloat16)
        scaled = (packed[:, width:] * inv_count).astype(jnp.bfloat16)
        (both,) = exchange(
            [jnp.concatenate([tok_rows, scaled], axis=1)], (("mp", "all"),), 1
        )
        both = both.transpose(1, 0, 2)
        tok_full = both[:, :, :width].reshape(chunk, model_width).astype(jnp.float32)
        scaled_full = both[:, :, width:].reshape(chunk, model_width)
        squares = jnp.sum(tok_full * tok_full, axis=1, keepdims=True)
        inv_rms = lax.rsqrt(squares / model_width + epsilon)
        normed_full = (tok_full * inv_rms * gain_full[None, :]).astype(jnp.bfloat16)
        pre_act = jnp.dot(normed_full, up_weight, preferred_element_type=jnp.float32)
        activated = gelu_tanh(pre_act).astype(jnp.bfloat16)
        grad_act = contract_cols(scaled_full, down_weight)
        grad_pre = jax.vjp(gelu_tanh, pre_act)[1](grad_act)[0].astype(jnp.bfloat16)

        by_cols = jnp.concatenate(
            [
                normed_full.reshape(chunk, n_dp, cols),
                scaled_full.reshape(chunk, n_dp, cols),
            ],
            axis=2,
        ).transpose(1, 0, 2)

        row_part = jnp.sum(grad_pre.astype(jnp.float32) * pre_act, axis=1, keepdims=True)
        partial = contract_cols(grad_pre, up_weight).astype(jnp.bfloat16)
        shares, row_parts = exchange(
            [
                partial.reshape(chunk, n_mp, width).transpose(1, 0, 2),
                jnp.broadcast_to(row_part / inv_rms, (chunk, 128)),
            ],
            (("mp", "split"), ("mp", "all")),
            2,
        )
        grad_normed = jnp.sum(shares.astype(jnp.float32), axis=0)
        row_dot = jnp.sum(row_parts, axis=0)[:, :1]
        values = tok_rows.astype(jnp.float32)
        cubed = inv_rms * inv_rms * inv_rms
        in_rows = (
            scaled.astype(jnp.float32)
            + norm_gain[None, :] * grad_normed * inv_rms
            - values * cubed * row_dot / model_width
        ).astype(jnp.bfloat16)
        gain_term = jnp.sum(grad_normed * values * inv_rms, axis=0)
        back = contract_rows(pick, in_rows).astype(jnp.bfloat16)
        act_all, pre_all, by_cols, back, gain_parts = exchange(
            [
                activated,
                grad_pre,
                by_cols,
                back.reshape(n_dp, micro * share, width),
                jnp.broadcast_to(gain_term[None, :], (8, width)),
            ],
            (("dp", "tree"), ("dp", "tree"), ("dp", "split"), ("dp", "split"), ("dp", "all")),
            3,
        )
        by_cols = by_cols.reshape(n_dp * chunk, 2 * cols)
        up_term = contract_rows(by_cols[:, :cols], pre_all.reshape(n_dp * chunk, ff_shard))
        down_term = contract_rows(act_all.reshape(n_dp * chunk, ff_shard), by_cols[:, cols:])
        return (back, up_term, down_term, jnp.sum(gain_parts[:, 0], axis=0))

    def add_chunk(index, total):
        return jax.tree.map(jnp.add, total, run_chunk(index))

    total = run_chunk(jnp.int32(0))
    back, up_grad, down_grad, gain_acc = lax.fori_loop(1, chunk_total, add_chunk, total)
    return (unstripe(back, micro), up_grad, down_grad, gain_acc)


def phase(name):
    return contextlib.nullcontext()


gelu_slope = 0.7978845608028654
gelu_cube = 0.044715
MESH = pl.DeviceIdType.MESH


def packed_chunk(slot_count):
    return -(-slot_count * 3 // 8 // 16) * 16


def dealing(micro, tok, n_dp):
    rows, share = micro * tok, tok // n_dp
    shift = share.bit_length() - 1
    line = lax.broadcasted_iota(jnp.int32, (rows, rows), 0)
    lane = lax.broadcasted_iota(jnp.int32, (rows, rows), 1)
    m_of = (line >> shift) & (micro - 1)
    d_of = line >> ((micro * share).bit_length() - 1)
    first = jnp.where((m_of & 1) == 1, n_dp - 1 - d_of, d_of)
    source = m_of * tok + (line & (share - 1)) * n_dp + first
    return (source == lane).astype(jnp.float32).astype(jnp.bfloat16)


def fused_kernel(
    hid, og, fill, gain, index, up_hbm, down_hbm,
    act_o, gp_o, ns_o, gs_o, back_o, terms_o, trips,
    upw, dnt, hbuf, gbuf, act, pre, normed, ns, gs, gp,
    sent_h, sent_g, got_h, got_g, fills_out, fill_send, gain_send, gain_full,
    part, shares, row_send, rows_in, term_send, terms_in,
    sent_back, got_back, perm, pick,
    w_sem, o_sem, h0_s, h0_r, g0_s, g0_r, f_s, f_r, n_s, n_r,
    ht_s, ht_r, gt_s, gt_r, p_s, p_r, q_s, q_r, b_s, b_r, t_s, t_r,
):
    n_dp, n_mp = lax.axis_size("dp"), lax.axis_size("mp")
    me, mine = lax.axis_index("dp"), lax.axis_index("mp")
    core = lax.rem(mine, 2)
    high = lax.div(mine, 2)
    low = lax.rem(me, 2)
    micro, tok, width = hid.shape
    model, ff = upw.shape
    rows = micro * tok
    share = tok // n_dp
    per = micro * share
    chunk = hbuf.shape[0] // n_dp
    cols = model // n_dp
    group = 2 * chunk
    zs = n_dp // 2
    tile = 256
    f32, bf16 = jnp.float32, jnp.bfloat16

    up_load = pltpu.make_async_copy(up_hbm, upw, w_sem.at[0])
    up_load.start()
    span = model // 2
    slots = zs * group // tile
    flips = [
        pltpu.make_async_copy(
            down_hbm.at[(i // 2) * tile : (i // 2 + 1) * tile, (i % 2) * span : (i % 2 + 1) * span],
            act.at[(i % slots) * tile : (i % slots + 1) * tile, 0:span],
            w_sem.at[1 + i % slots],
        )
        for i in range(2 * ff // tile)
    ]
    for flip in flips[:slots]:
        flip.start()

    barrier = pltpu.get_barrier_semaphore()
    for axis, n, at in (("dp", n_dp, me), ("mp", n_mp, mine)):
        for d in range(1, n):
            pl.semaphore_signal(
                barrier, inc=1, device_id={axis: lax.rem(at + d, n)}, device_id_type=MESH
            )

    shift = share.bit_length() - 1
    perm[...] = dealing(micro, tok, n_dp)

    def deal(block, target):
        total = 0.0
        for m in range(micro):
            total = total + jnp.dot(
                perm[:, m * tok : (m + 1) * tok], block[m], preferred_element_type=f32
            )
        target[...] = total.astype(bf16)

    deal(hid, sent_h)
    ids = lax.broadcasted_iota(jnp.int32, fill_send.shape, 0)
    tile_fill = jnp.zeros(fill_send.shape, jnp.int32)
    for m in range(micro):
        tile_fill = jnp.where(ids == m, fill[0, m], tile_fill)
    fill_send[...] = tile_fill
    gain_row = gain[...].reshape(1, width)
    gain_send[...] = jnp.broadcast_to(gain_row, gain_send.shape)

    with phase("barrier"):
        pl.semaphore_wait(barrier, n_dp + n_mp - 2)

    def remote(src, dst, s_sem, r_sem, device):
        return pltpu.make_async_remote_copy(
            src_ref=src, dst_ref=dst, send_sem=s_sem, recv_sem=r_sem,
            device_id=device, device_id_type=MESH,
        )

    def to_dp(source_of, target, s_sems, r_sems):
        out = []
        for d in [n_dp // 2] + [d for d in range(1, n_dp) if d != n_dp // 2]:
            peer = lax.rem(me + d, n_dp)
            out.append(remote(source_of(peer), target, s_sems.at[d], r_sems.at[d], {"dp": peer}))
        return out

    def to_mp(source_of, target, s_sems, r_sems):
        out = []
        for d in range(1, n_mp):
            peer = lax.rem(mine + d, n_mp)
            out.append(remote(source_of(peer), target, s_sems.at[d], r_sems.at[d], {"mp": peer}))
        return out

    def start(copies):
        for copy in copies:
            copy.start()

    def received(copies):
        for copy in copies:
            copy.wait_recv()

    def slot(ref, r):
        return ref.at[pl.ds(pl.multiple_of(r * per, per), per), :]

    def strip(q):
        return pl.ds(pl.multiple_of(q * width, 128), width)

    def rank_rows(r):
        return pl.ds(pl.multiple_of(r * chunk, 16), chunk)

    fill_copies = to_dp(lambda peer: fill_send, fills_out.at[me], f_s, f_r)
    h_copies = to_dp(lambda peer: slot(sent_h, peer), slot(got_h, me), h0_s, h0_r)
    gain_copies = to_mp(lambda peer: gain_send, gain_full.at[:, strip(mine)], n_s, n_r)
    g_copies = to_dp(lambda peer: slot(sent_g, peer), slot(got_g, me), g0_s, g0_r)
    part_copies = to_mp(lambda peer: part.at[:, strip(peer)], shares.at[mine], p_s, p_r)
    part_copies += to_mp(lambda peer: row_send, rows_in.at[mine], q_s, q_r)
    back_copies = to_dp(lambda peer: slot(sent_back, peer), slot(got_back, me), b_s, b_r)
    back_copies += to_dp(lambda peer: term_send, terms_in.at[me], t_s, t_r)
    start(fill_copies)
    start(h_copies)
    start(gain_copies)
    here = pl.ds(pl.multiple_of(me * per, per), per)
    got_h[here, :] = sent_h[here, :]
    fills_out[me] = fill_send[...]
    gain_full[:, strip(mine)] = gain_send[...]

    deal(og, sent_g)

    with phase("flips"):
        for i, flip in enumerate(flips):
            flip.wait()
            held = slice((i % slots) * tile, (i % slots + 1) * tile)
            for j in range(span // tile):
                to = slice((i % 2) * span + j * tile, (i % 2) * span + (j + 1) * tile)
                dnt[to, (i // 2) * tile : (i // 2 + 1) * tile] = act[
                    held, j * tile : (j + 1) * tile
                ].T
            if i + slots < len(flips):
                flips[i + slots].start()
    with phase("fills"):
        received(fill_copies)
    lanes = lax.broadcasted_iota(jnp.int32, (1, rows), 1)
    count = jnp.zeros((1, rows), jnp.int32)
    token_total = jnp.zeros((1, 1), jnp.int32)
    for r in range(n_dp):
        for m in range(micro):
            one = fills_out[r, m : m + 1, 0:1]
            token_total = token_total + one
            count = jnp.where((lanes >> shift) == r * micro + m, one, count)
    odd = (lanes >> shift) & 1
    begin = jnp.where(odd == 1, n_dp - 1 - me, me)
    live = begin + (lanes & (share - 1)) * n_dp < count
    inv_count = 1.0 / token_total.astype(f32)
    ranks = lax.broadcasted_iota(jnp.int32, (1, 128), 1)
    load = jnp.zeros((1, 128), jnp.int32)
    for r in range(n_dp):
        for m in range(micro):
            off = n_dp - 1 - ranks if m % 2 else ranks
            some = (fills_out[r, m : m + 1, :] - off + n_dp - 1) >> (n_dp.bit_length() - 1)
            load = load + jnp.minimum(jnp.maximum(some, 0), share)
    load = jnp.where(ranks < n_dp, load, 0)
    steps = jnp.zeros((1, 128), jnp.int32)
    for i in range(-(-rows // chunk)):
        steps = steps + (load > i * chunk).astype(jnp.int32)
    trips[0] = jnp.max(steps)
    live_f = live.astype(f32)
    line = lax.broadcasted_iota(jnp.int32, (rows, rows), 0)
    lane = lax.broadcasted_iota(jnp.int32, (rows, rows), 1)
    upto = (line < lane).astype(f32).astype(bf16)
    place = jnp.dot(
        jnp.broadcast_to(live_f, (16, rows)).astype(bf16), upto, preferred_element_type=f32
    )[0:1, :]
    place = jnp.where(live, place, -1.0)
    spots = (lax.broadcasted_iota(jnp.int32, (chunk, rows), 0) + index[0] * chunk).astype(f32)
    pick[...] = (spots == place).astype(f32).astype(bf16)

    def along(at_dp, at_mp, x, y):
        return (
            at_dp + x - 2 * x * lax.rem(at_dp, 2),
            at_mp + 2 * y - 4 * y * lax.div(at_mp, 2),
        )

    def owner(t, at_mp, c):
        t1, t0 = (t >> 1) & 1, t & 1
        x = t1 * (1 - c) + t0 * c
        y = t0 * (1 - c) + t1 * c
        return along(flipped_by(me, (t >> 2) * 2), at_mp, x, y)

    def toward(bit):
        if bit >= 4:
            return flipped(me, bit // 2), mine
        if bit == 2:
            return along(me, mine, 1 - core, core)
        return along(me, mine, core, 1 - core)

    nodes = 2 * n_dp
    top = n_dp
    partner = mine + 1 - 2 * core
    trees = {"h": (hbuf, ht_s, ht_r), "g": (gbuf, gt_s, gt_r)}

    def hop(k, t):
        buf, s_sems, r_sems = trees[k]
        if t >= nodes:
            dp_o, mp_o = owner(t - nodes, mine, core)
            device = {"mp": partner}
        else:
            dp_o, mp_o = owner(t & (t - 1), mine, core)
            dp_t, mp_t = toward(t & -t)
            device = {"dp": dp_t, "mp": mp_t}
        block = buf.at[rank_rows(dp_o), strip(mp_o)]
        return remote(block, block, s_sems.at[t], r_sems.at[t], device)

    def forward(k, t):
        bit = (t & -t) // 2 if t else top
        while bit >= 1:
            hop(k, t ^ bit).start()
            bit //= 2
        hop(k, nodes + t).start()

    def arrive(k, *ts):
        for t in ts:
            hop(k, t).wait_recv()
            forward(k, t)

    def joined(k, z):
        for t in range(4 * z, 4 * z + 4):
            hop(k, nodes + t).wait_recv()

    def base_of(z):
        at, out, bit = lax.div(me, 2), 0, 1
        while bit < zs:
            a, b = lax.rem(lax.div(at, bit), 2), lax.rem(lax.div(z, bit), 2)
            out = out + bit * (a + b - 2 * a * b)
            bit *= 2
        return 2 * out

    half = lax.div(me, n_dp // n_mp)
    part_at = lax.rem(me, n_dp // n_mp)

    def slice_cols(value):
        out = value[:, 0:cols]
        for i in range(1, n_dp // n_mp):
            out = jnp.where(part_at == i, value[:, i * cols : (i + 1) * cols], out)
        return out

    def rms(block):
        return lax.rsqrt(jnp.sum(block * block, axis=1, keepdims=True) / model + epsilon)

    tiles = [slice(n * tile, (n + 1) * tile) for n in range(ff // tile)]
    mid = (len(tiles) + 1) // 2
    pieces = [tiles[:mid], tiles[mid:]]

    def keep(z, pairs, at):
        held = pl.ds(pl.multiple_of(z * group, 64), group)
        return [
            pltpu.make_async_copy(ref.at[held, :], out.at[held, :], o_sem.at[at + n, z])
            for n, (ref, out) in enumerate(pairs)
        ]

    def keep_pre(z):
        return keep(z, ((act, act_o), (ns, ns_o)), 0)

    def keep_grad(z):
        return keep(z, ((gp, gp_o), (gs, gs_o)), 2)

    def do_pre(z, between):
        base = base_of(z)
        held = pl.ds(pl.multiple_of(z * group, 64), group)

        def norm_rows(i, carry):
            for k in range(4):
                src = pl.ds(pl.multiple_of(base * chunk + i * 64 + k * 16, 16), 16)
                dst = pl.ds(pl.multiple_of(i * 64 + k * 16, 16), 16)
                value = hbuf[src, :].astype(f32)
                normed[dst, :] = (value * rms(value) * gain_full[0:1, :]).astype(bf16)
            return carry

        with phase("norm"):
            lax.fori_loop(0, group // 64, norm_rows, 0)
            ns[held, :] = slice_cols(normed[:, strip(half)].astype(f32)).astype(bf16)
        for n, some in enumerate(pieces):
            between(n)
            with phase("pre_tiles"):
                for at in some:
                    value = jnp.dot(normed[...], upw[:, at], preferred_element_type=f32)
                    pre[z, :, at] = value
                    bent = jnp.tanh(
                        gelu_slope * (value + gelu_cube * (value * value * value))
                    )
                    act[held, at] = (value * (0.5 * (1.0 + bent))).astype(bf16)
        for copy in keep_pre(z):
            copy.start()

    def do_grad(z, between):
        base = base_of(z)
        block = pl.ds(pl.multiple_of(base * chunk, 16), group)
        held = pl.ds(pl.multiple_of(z * group, 64), group)
        with phase("gslice"):
            gs[held, :] = slice_cols(gbuf[block, strip(half)].astype(f32)).astype(bf16)
        for n, some in enumerate(pieces):
            between(n)
            with phase("grad_tiles"):
                for at in some:
                    grad = jnp.dot(gbuf[block, :], dnt[:, at], preferred_element_type=f32)
                    value = pre[z, :, at]
                    square = value * value
                    bent = jnp.tanh(gelu_slope * (value + gelu_cube * (square * value)))
                    slope = 0.5 * (1.0 + bent) + (0.5 * value) * (1.0 - bent * bent) * (
                        gelu_slope * (1.0 + 3.0 * gelu_cube * square)
                    )
                    gp[held, at] = (grad * slope).astype(bf16)
        for copy in keep_grad(z):
            copy.start()

    def compact(got, buf, scale):
        packed = jnp.dot(pick[...], got[...], preferred_element_type=f32)
        if scale is not None:
            packed = packed * scale
        buf[rank_rows(me), strip(mine)] = packed.astype(bf16)

    own = pl.ds(pl.multiple_of(low * chunk, 16), chunk)

    def own_parts():
        own_gp = gp[own, :]
        row_part = jnp.sum(own_gp.astype(f32) * pre[0, own, :], axis=1, keepdims=True)
        inv_rms = rms(hbuf[rank_rows(me), :].astype(f32))
        row_send[...] = jnp.broadcast_to(row_part / inv_rms, row_send.shape)
        for n in range(model // tile):
            at = slice(n * tile, (n + 1) * tile)
            if n % 7 == 0:
                run(own_events[n // 7])
            with phase("part_tiles"):
                part[:, at] = contract_cols(gp[own, :], upw[at, :]).astype(bf16)
        start(part_copies)

    def own_rows():
        with phase("part_wait"):
            received(part_copies)
        inv_rms = rms(hbuf[rank_rows(me), :].astype(f32))
        grad_normed = part[:, strip(mine)].astype(f32)
        row_dot = row_send[:, 0:1]
        for d in range(1, n_mp):
            peer = lax.rem(mine + d, n_mp)
            grad_normed = grad_normed + shares[peer].astype(f32)
            row_dot = row_dot + rows_in[peer][:, 0:1]
        values = hbuf[rank_rows(me), strip(mine)].astype(f32)
        scaled = gbuf[rank_rows(me), strip(mine)].astype(f32)
        cubed = inv_rms * inv_rms * inv_rms
        in_rows = (
            scaled + gain_row * grad_normed * inv_rms - values * (cubed * row_dot / model)
        ).astype(bf16)
        gain_term = jnp.sum(grad_normed * values * inv_rms, axis=0, keepdims=True)
        term_send[...] = jnp.broadcast_to(gain_term, term_send.shape)
        terms_in[me] = term_send[...]
        sent_back[...] = contract_rows(pick[...], in_rows).astype(bf16)
        got_back[here, :] = sent_back[here, :]
        start(back_copies)

    with phase("h_wait"):
        received(h_copies)
    with phase("start_h"):
        compact(got_h, hbuf, None)
        forward("h", 0)
    with phase("gain_wait"):
        received(gain_copies)

    def begin_g():
        start(g_copies)
        got_g[here, :] = sent_g[here, :]

    def pack_g():
        with phase("g_wait"):
            received(g_copies)
        with phase("start_g"):
            compact(got_g, gbuf, inv_count)
            forward("g", 0)

    def run(events):
        for event in events:
            if callable(event):
                event()
            elif event[0] == "j":
                with phase("join_" + event):
                    joined(event[1], int(event[2:]))
            else:
                with phase(event):
                    arrive(event[0], int(event[1:]))

    own_events = (["g10", "g6"], ["g5", "g9"])
    pre_events = {
        0: (["h2", "h1", "h4", "h8", begin_g, "h3", up_load.wait, "jh0"], ["h12"], []),
        1: (["h10", "h6", "h5", "h9", pack_g, "h7", "jh1"], ["h14"], ["g2", "g1"]),
        2: (["jh2"], ["g14"], ["g7"]),
        3: (["g11", "jh3"], ["g13"], ["g15"]),
    }
    grad_events = {
        0: (["g8", "g4", "h11", "h13", "g3", "jg0"], ["h15"], ["g12"]),
        1: (["jg1"], [], []),
        2: ([own_rows, "jg2"], [], []),
        3: (["jg3"], [], []),
    }

    def at_step(table, i, n):
        for z in range(zs):
            if table[z][n]:
                pl.when(i == z)(lambda z=z: run(table[z][n]))

    turn = zs // 2

    def step(i, carry):
        @pl.when(jnp.logical_or(i < turn, jnp.logical_and(i > turn, i <= zs)))
        def _():
            z = i - i // (turn + 1)
            at_step(pre_events, z, 0)
            do_pre(z, lambda n: at_step(pre_events, z, n + 1))

        @pl.when(jnp.logical_or(i == turn, i > zs))
        def _():
            z = (i - turn) * (i // (zs + 1)) - turn * (i // (zs + 1))
            at_step(grad_events, z, 0)
            do_grad(z, lambda n: at_step(grad_events, z, n + 1))

            @pl.when(i == turn)
            def _():
                own_parts()

        return carry

    lax.fori_loop(0, 2 * zs, step, 0)

    with phase("back_wait"):
        received(back_copies)
    lasts = [
        pltpu.make_async_copy(got_back, back_o, o_sem.at[4, 0]),
        pltpu.make_async_copy(terms_in, terms_o, o_sem.at[4, 1]),
    ]
    start(lasts)
    with phase("keeps_wait"):
        for z in range(zs):
            for copy in keep_pre(z) + keep_grad(z):
                copy.wait()
        for copy in lasts:
            copy.wait()
    with phase("sends_wait"):
        for copies in (fill_copies, h_copies, gain_copies, g_copies, part_copies, back_copies):
            for copy in copies:
                copy.wait_send()
        for k in ("h", "g"):
            for t in range(1, 2 * nodes):
                hop(k, t).wait_send()


def fused_call(hidden_in, out_grad, pack_fill, norm_gain, index, up_weight, down_weight):
    micro, tok, width = hidden_in.shape
    model, ff = up_weight.shape
    n_dp, n_mp = lax.axis_size("dp"), lax.axis_size("mp")
    rows = micro * tok
    per = rows // n_dp
    chunk = packed_chunk(rows)
    cols = model // n_dp
    group = 2 * chunk
    zs = n_dp // 2
    f32, bf16 = jnp.float32, jnp.bfloat16
    vmem = pl.BlockSpec(memory_space=pltpu.VMEM)
    smem = pl.BlockSpec(memory_space=pltpu.SMEM)
    hbm = pl.BlockSpec(memory_space=pl.ANY)
    dma = pltpu.SemaphoreType.DMA
    return pl.pallas_call(
        fused_kernel,
        out_shape=[
            jax.ShapeDtypeStruct((zs * group, ff), bf16),
            jax.ShapeDtypeStruct((zs * group, ff), bf16),
            jax.ShapeDtypeStruct((zs * group, cols), bf16),
            jax.ShapeDtypeStruct((zs * group, cols), bf16),
            jax.ShapeDtypeStruct((rows, width), bf16),
            jax.ShapeDtypeStruct((n_dp, 8, width), f32),
            jax.ShapeDtypeStruct((1,), jnp.int32),
        ],
        in_specs=[vmem, vmem, smem, vmem, smem, hbm, hbm],
        out_specs=[hbm] * 6 + [smem],
        scratch_shapes=[
            pltpu.VMEM((model, ff), bf16),
            pltpu.VMEM((model, ff), bf16),
            pltpu.VMEM((n_dp * chunk, model), bf16),
            pltpu.VMEM((n_dp * chunk, model), bf16),
            pltpu.VMEM((zs * group, ff), bf16),
            pltpu.VMEM((zs, group, ff), f32),
            pltpu.VMEM((group, model), bf16),
            pltpu.VMEM((zs * group, cols), bf16),
            pltpu.VMEM((zs * group, cols), bf16),
            pltpu.VMEM((zs * group, ff), bf16),
            pltpu.VMEM((rows, width), bf16),
            pltpu.VMEM((rows, width), bf16),
            pltpu.VMEM((rows, width), bf16),
            pltpu.VMEM((rows, width), bf16),
            pltpu.VMEM((n_dp, 8, 128), jnp.int32),
            pltpu.VMEM((8, 128), jnp.int32),
            pltpu.VMEM((8, width), f32),
            pltpu.VMEM((8, model), f32),
            pltpu.VMEM((chunk, model), bf16),
            pltpu.VMEM((n_mp, chunk, width), bf16),
            pltpu.VMEM((chunk, 128), f32),
            pltpu.VMEM((n_mp, chunk, 128), f32),
            pltpu.VMEM((8, width), f32),
            pltpu.VMEM((n_dp, 8, width), f32),
            pltpu.VMEM((rows, width), bf16),
            pltpu.VMEM((rows, width), bf16),
            pltpu.VMEM((rows, rows), bf16),
            pltpu.VMEM((chunk, rows), bf16),
            dma((8,)),
            dma((5, zs)),
        ]
        + [dma((n_dp,))] * 6
        + [dma((n_mp,))] * 2
        + [dma((4 * n_dp,))] * 4
        + [dma((n_mp,))] * 4
        + [dma((n_dp,))] * 4,
        compiler_params=pltpu.CompilerParams(
            collective_id=7, has_side_effects=True, vmem_limit_bytes=67043328
        ),
        cost_estimate=pl.CostEstimate(
            flops=8 * rows * model * ff, bytes_accessed=6 * model * ff, transcendentals=0
        ),
    )(hidden_in, out_grad, pack_fill.T, norm_gain, index, up_weight, down_weight)


def finish_kernel(
    act, gp, ns, gs, back, terms, in_part, up_out, down_out, gain_out, nst, gst
):
    @pl.when(pl.program_id(0) == 0)
    def _():
        nst[...] = ns[...].T
        gst[...] = gs[...].T
        micro, tok, width = in_part.shape
        n_dp = terms.shape[0]
        perm = dealing(micro, tok, n_dp)
        for m in range(micro):
            in_part[m] = contract_rows(perm[:, m * tok : (m + 1) * tok], back[...]).astype(
                jnp.bfloat16
            )
        gain_out[...] = jnp.sum(terms[...], axis=0)[0:1].reshape(width)

    up_out[...] = jnp.dot(nst[...], gp[...], preferred_element_type=jnp.float32)
    down_out[...] = jnp.dot(gst[...], act[...], preferred_element_type=jnp.float32)


def finish_call(act, gp, ns, gs, back, terms, micro):
    total, ff = act.shape
    cols = ns.shape[1]
    rows, width = back.shape
    tok = rows // micro
    tile = 256
    f32, bf16 = jnp.float32, jnp.bfloat16

    def whole(shape):
        return pl.BlockSpec(shape, lambda n: (0,) * len(shape))

    def strips(height):
        return pl.BlockSpec((height, tile), lambda n: (0, n))

    return pl.pallas_call(
        finish_kernel,
        grid=(ff // tile,),
        out_shape=[
            jax.ShapeDtypeStruct((micro, tok, width), bf16),
            jax.ShapeDtypeStruct((cols, ff), f32),
            jax.ShapeDtypeStruct((cols, ff), f32),
            jax.ShapeDtypeStruct((width,), f32),
        ],
        in_specs=[
            strips(total), strips(total), whole(ns.shape), whole(gs.shape),
            whole(back.shape), whole(terms.shape),
        ],
        out_specs=[whole((micro, tok, width)), strips(cols), strips(cols), whole((width,))],
        scratch_shapes=[pltpu.VMEM((cols, total), bf16), pltpu.VMEM((cols, total), bf16)],
        compiler_params=pltpu.CompilerParams(vmem_limit_bytes=67043328),
    )(act, gp, ns, gs, back, terms)


def on_device_fused(hidden_in, out_grad, pack_fill, norm_gain, up_weight, down_weight):
    def run_chunk(index):
        *parts, trips = fused_call(
            hidden_in, out_grad, pack_fill, norm_gain,
            jnp.reshape(index, (1,)).astype(jnp.int32), up_weight, down_weight,
        )
        return finish_call(*parts, hidden_in.shape[0]), trips

    total, trips = run_chunk(jnp.int32(0))

    def add_chunk(index, so_far):
        more, _ = run_chunk(index)
        return jax.tree.map(jnp.add, so_far, more)

    in_grad, up_grad, down_grad, gain = lax.fori_loop(1, trips[0], add_chunk, total)
    return (in_grad, up_grad, down_grad.T, gain)


def solution(mesh):
    in_specs = (
        P(None, "dp", "mp"),
        P(None, "dp", "mp"),
        P(None, "dp"),
        P("mp"),
        P(None, "mp"),
        P("mp", None),
    )
    out_specs = (P(None, "dp", "mp"), P("dp", "mp"), P("mp", "dp"), P("mp"))

    def local(hidden_in, out_grad, pack_fill, norm_gain, up_weight, down_weight):
        micro, tok, width = hidden_in.shape
        n_dp, n_mp = mesh.shape["dp"], mesh.shape["mp"]
        share = tok // n_dp
        fits = (
            (n_dp, n_mp, micro) == (8, 4, 2)
            and width % 128 == 0
            and up_weight.shape[1] % 256 == 0
            and up_weight.shape[0] % 256 == 0
            and tok % 128 == 0
            and share & (share - 1) == 0
        )
        body = on_device_fused if fits else on_device
        return body(hidden_in, out_grad, pack_fill, norm_gain, up_weight, down_weight)

    return jax.shard_map(
        local, mesh=mesh, in_specs=in_specs, out_specs=out_specs, check_vma=False
    )
```
